1024 devices in a mesh: tile: 4 (over y_lo), seq: 8 (over z), group: 32 (over x, y_hi, core).
Axes of the slice: x: 8, y: 8 (y_hi: 2, y_lo: 4; y = y_hi * 4 + y_lo), z: 8, core: 2. Of those that a mesh axis runs over, the one named last changes fastest.
Arguments:
- features: bfloat16 [8, 32, 2, 16, 64, 512], P('seq', 'group', None, 'tile'), may hold values from -6 to 6
- conv_weight: bfloat16 [3, 3, 3, 512, 16], replicated, may hold values from -0.0546875 to 0.0546875
- conv_bias: float32 [16], replicated, may hold values from -3 to 3
- embed_qkv: bfloat16 [64, 4608], replicated, may hold values from -0.75 to 0.75
- query_gain: float32 [128], replicated, may hold values from 0.5 to 2
- key_gain: float32 [128], replicated, may hold values from 0.5 to 2
- bucket: int32 [8, 32], replicated, may hold values from 0 to 31, as said below
- frames: int32 [8, 32], replicated, may hold values from 1 to 2
Outputs:
- attended: bfloat16 [8, 32, 2, 512, 1536], P('seq', 'group', None, 'tile')
The draws below stay inside these ranges and needn't reach their ends.
Inputs may be any that keep to these rules, and one draw needn't show every extreme that they name: In each row every bucket receives at most 2 clips; exactly 8 buckets receive 2, and as many receive none.
All inputs are finite; a program needn't handle non-finite values.
Results may differ from the reference program's by a relative error of at most 0.0046.
Values may be sent and summed in bfloat16 or wider, within the bound.
A program may use at most 128 MiB of HBM per device.

```python
import math
import jax
import jax.numpy as jnp
from jax import lax

HEADS = 12
HEAD = 128
D = 1536
CH = 512
ZC = 16
TL = 2
HL = 4
WL = 64
CAP = 2
TOK = 128
TOKC = 512
N_TILE = 4
N_SEQ = 8
N_GROUP = 32


def draw_bucket(key, part):

    def one_row(row_key):
        first_key, second_key = jax.random.split(row_key)
        ranking = jax.random.permutation(first_key, N_GROUP)
        targets = jax.random.permutation(second_key, N_GROUP)
        paired = N_GROUP // 4
        position = jnp.where(ranking < 2 * paired, ranking // 2, ranking - paired)
        return targets[position]
    row_keys = jax.random.split(jax.random.fold_in(key, 7), N_SEQ)
    return jax.vmap(one_row)(row_keys).astype(jnp.int32)


def set_ends(array, rng, least, top_value):
    dims = array.shape
    index_at = [jax.random.randint(jax.random.fold_in(rng, axis), (), 0, dims[axis]) for axis in range(len(dims))]
    array = array.at[tuple(index_at)].set(least)
    longest = dims.index(max(dims))
    index_at[longest] = (index_at[longest] + 1) % dims[longest]
    return array.at[tuple(index_at)].set(top_value)


def steps_of(stream_key, dims, cuts, least, largest):
    gain = 1.0
    for axis_at, shards_of in cuts:
        steps = jax.random.uniform(jax.random.fold_in(jax.random.fold_in(stream_key, 6), axis_at), (shards_of,), jnp.float32, least / len(cuts), largest / len(cuts))
        gain = gain * jnp.repeat(jnp.exp(steps), dims[axis_at] // shards_of).reshape((-1,) + (1,) * (len(dims) - 1 - axis_at))
    return gain


def normal_values(stream_key, extent, width, bound, shards=(), kind=jnp.bfloat16):
    values = width * jax.random.normal(stream_key, extent, jnp.float32)
    if shards:
        values = values * steps_of(stream_key, extent, shards, -0.22, 0.18)
    return jnp.clip(values, -bound, bound).astype(kind)


def setup_inputs(seed: int = 0) -> dict:
    splits = jax.random.split(jax.random.key(seed), 9)
    return {
        "features": normal_values(splits[0], (N_SEQ, N_GROUP, TL, N_TILE * HL, WL, CH), 1.0, 6.0, ((0, 8), (1, 32), (3, 4))),
        "conv_weight": normal_values(splits[1], (3, 3, 3, CH, ZC), (27 * CH) ** -0.5, 0.0546875),
        "conv_bias": normal_values(splits[2], (ZC,), 0.5, 3.0, (), jnp.float32),
        "embed_qkv": normal_values(splits[3], (4 * ZC, 3 * D), (4 * ZC) ** -0.5, 0.75),
        "query_gain": jnp.clip(jnp.exp(jax.random.uniform(splits[4], (HEAD,), jnp.float32, math.log(0.5), math.log(2.0))), 0.5, 2.0),
        "key_gain": jnp.clip(jnp.exp(jax.random.uniform(splits[5], (HEAD,), jnp.float32, math.log(0.5), math.log(2.0))), 0.5, 2.0),
        "bucket": draw_bucket(jax.random.fold_in(splits[8], 71), 0),
        "frames": set_ends(jax.random.randint(splits[7], (N_SEQ, N_GROUP), 1, TL + 1), jax.random.fold_in(splits[7], 1), 1, TL).astype(jnp.int32),
    }


def tap_products(padded, conv_weight):
    channels = padded.shape[-1]
    flat_weight = jnp.transpose(conv_weight, (3, 0, 1, 2, 4)).reshape(channels, -1)
    products = jnp.dot(padded.reshape(-1, channels), flat_weight, preferred_element_type=jnp.float32)
    return products.reshape(padded.shape[:-1] + (27, conv_weight.shape[-1]))

def tap_sum(products, frame_count, row_count, col_count):
    running = jnp.zeros((frame_count, row_count, col_count, products.shape[-1]), jnp.float32)
    for depth_tap in range(3):
        for row_tap in range(3):
            for col_tap in range(3):
                tap_index = depth_tap * 9 + row_tap * 3 + col_tap
                running = running + products[depth_tap:depth_tap + frame_count, row_tap:row_tap + row_count, col_tap:col_tap + col_count, tap_index]
    return running

def head_norm(values, gain_vec, head_size):
    shaped = values.reshape(values.shape[:-1] + (-1, head_size))
    scaled = shaped * lax.rsqrt(lax.optimization_barrier(jnp.mean(shaped * shaped, axis=-1, keepdims=True)) + 1e-06)
    return scaled * gain_vec

def attend(queries, key_rows, value_rows, key_valid):
    query_wide = lax.optimization_barrier(queries).astype(jnp.float32)
    key_wide = lax.optimization_barrier(key_rows).astype(jnp.float32)
    value_wide = lax.optimization_barrier(value_rows).astype(jnp.float32)
    scores = jnp.einsum('qhe,khe->hqk', query_wide, key_wide)
    scores = jnp.where(key_valid[None, None, :], scores, -1e+30)
    row_max = lax.optimization_barrier(jnp.max(scores, axis=-1, keepdims=True))
    weights = jnp.exp(scores - row_max)
    totals = lax.optimization_barrier(jnp.sum(weights, axis=-1))
    weight_low = lax.optimization_barrier(weights.astype(jnp.bfloat16)).astype(jnp.float32)
    mixed_out = jnp.einsum('hqk,khe->qhe', weight_low, value_wide)
    return mixed_out / jnp.transpose(totals)[:, :, None]

def reference(features, conv_weight, conv_bias, embed_qkv, query_gain, key_gain, bucket, frames):
    clips = features.reshape((N_SEQ * N_GROUP,) + features.shape[2:])

    def encode_attend(pair):
        clip_block, frame_total = pair
        padded = jnp.pad(clip_block, ((2, 0), (1, 1), (1, 1), (0, 0)), mode='edge')
        summed = tap_sum(tap_products(padded, conv_weight), TL, N_TILE * HL, WL)
        latent = (summed + conv_bias).astype(jnp.bfloat16)
        tokens = latent.reshape(TL, N_TILE, HL // 2, 2, WL // 2, 2, ZC)
        tokens = jnp.transpose(tokens, (1, 0, 2, 4, 3, 5, 6)).reshape(-1, 4 * ZC)
        projected = jnp.dot(tokens, embed_qkv, preferred_element_type=jnp.float32)
        queries = (head_norm(projected[:, :D], query_gain, HEAD) / math.sqrt(HEAD)).astype(jnp.bfloat16)
        key_rows = head_norm(projected[:, D:2 * D], key_gain, HEAD).astype(jnp.bfloat16)
        value_rows = projected[:, 2 * D:].reshape(-1, HEADS, HEAD).astype(jnp.bfloat16)
        frame_of = jnp.arange(TOKC, dtype=jnp.int32) % TOK // (HL // 2 * (WL // 2))
        valid = frame_of < frame_total
        mixed_out = attend(queries, key_rows, value_rows, valid)
        return jnp.where(valid[:, None], mixed_out.reshape(-1, D), 0.0).astype(jnp.bfloat16)
    results = lax.map(encode_attend, (clips, frames.reshape(-1)))
    order_ids = jnp.arange(N_GROUP, dtype=jnp.int32)
    same_bucket = bucket[:, :, None] == bucket[:, None, :]
    earlier = order_ids[None, None, :] < order_ids[None, :, None]
    slot_of = lax.optimization_barrier(jnp.sum(jnp.where(same_bucket & earlier, 1, 0), axis=2)).astype(jnp.int32)
    slot_ids = jnp.arange(CAP, dtype=jnp.int32)
    matches = (bucket[:, None, None, :] == order_ids[None, :, None, None]) & (slot_of[:, None, None, :] == slot_ids[None, None, :, None])
    source = lax.optimization_barrier(jnp.sum(jnp.where(matches, order_ids[None, None, None, :], 0), axis=3)).astype(jnp.int32)
    present = jnp.any(matches, axis=3)
    flat_index = (jnp.arange(N_SEQ, dtype=jnp.int32)[:, None, None] * N_GROUP + source).astype(jnp.int32)
    placed = results[flat_index]
    return jnp.where(present[:, :, :, None, None], placed, jnp.zeros((), jnp.bfloat16))
```

```python
import math

import jax
import jax.numpy as jnp
from jax import lax
from jax.experimental import pallas as pl
from jax.experimental.pallas import tpu as pltpu
from jax.sharding import PartitionSpec as P

HEADS = 12
HEAD = 128
D = 1536
CAP = 2
N_X = 8
ZC = 16
MESH = pl.DeviceIdType.MESH
STEPS = 3
PER_STEP = HEADS // STEPS


def dot(a, b, dims=((1,), (0,))):
    return lax.dot_general(a, b, (dims, ((), ())), preferred_element_type=jnp.float32)


def route_kernel(feat_hbm, weight_hbm, bias, bucket, out, feat, weight, halo_out, halo_in,
                 xbuf, pick_out, pick_in, ysum, ybuf,
                 load_sem, halo_ssem, halo_rsem, x_ssem, x_rsem, c_ssem, c_rsem, y_ssem, y_rsem):
    tile = lax.axis_index("tile")
    seq = lax.axis_index("seq")
    group = lax.axis_index("group")
    n_tile = lax.axis_size("tile")
    x_at = group // 4
    hi_at = (group // 2) % 2
    core_at = group % 2

    def at_x(step):
        return {"group": ((x_at + step) % N_X) * 4 + hi_at * 2 + core_at}

    def at_y(step_hi, step_tile):
        return {"tile": (tile + step_tile) % n_tile,
                "group": x_at * 4 + ((hi_at + step_hi) % 2) * 2 + core_at}

    partner = {"group": x_at * 4 + hi_at * 2 + (1 - core_at)}
    y_steps = [(1, 0), (1, 1), (1, 3), (1, 2), (0, 2), (0, 1), (0, 3)]

    barrier = pltpu.get_barrier_semaphore()
    for step in (4, 3, 5, 2, 6, 1, 7):
        pl.semaphore_signal(barrier, inc=1, device_id=at_x(step), device_id_type=MESH)
    for step in y_steps:
        pl.semaphore_signal(barrier, inc=1, device_id=at_y(*step), device_id_type=MESH)
    pl.semaphore_signal(barrier, inc=1, device_id=partner, device_id_type=MESH)

    load_weight = pltpu.make_async_copy(weight_hbm, weight, load_sem.at[0])
    load_feat = pltpu.make_async_copy(feat_hbm, feat, load_sem.at[1])
    load_weight.start()
    load_feat.start()
    xbuf[N_X] = jnp.zeros((64, 128), jnp.bfloat16)

    buckets = [x_at * 4 + ((hi_at + d_hi) % 2) * 2 + (core_at + d_core) % 2
               for d_hi in range(2) for d_core in range(2)]

    def scan_slot(g, carry):
        here = bucket[seq, g]
        done = []
        for at, wanted in enumerate(buckets):
            first, second, count = carry[3 * at : 3 * at + 3]
            hit = here == wanted
            first = jnp.where(hit & (count == 0), g, first)
            second = jnp.where(hit & (count == 1), g, second)
            count = count + jnp.where(hit, 1, 0)
            done += [first, second, count]
        return tuple(done)

    slots = lax.fori_loop(0, 32, scan_slot, (jnp.int32(0),) * 12)

    load_weight.wait()
    load_feat.wait()

    taps = weight[...]
    first_frame = feat[0].reshape(256, 512)
    second_frame = feat[1].reshape(256, 512)
    from_first = dot(taps, first_frame, ((1,), (1,)))
    from_second = dot(taps[288:], second_frame, ((1,), (1,)))
    both = from_first[:144] + from_first[144:288]
    frame_sums = (both + from_first[288:], both + from_second)

    lane = lax.broadcasted_iota(jnp.int32, (ZC, 128), 1)
    column = lane % 64
    low_half = lane < 64

    def columns(sums, row_tap, pair):
        def at(col_tap):
            begin = (row_tap * 3 + col_tap) * ZC
            return sums[begin : begin + ZC, pair * 128 : pair * 128 + 128]

        left, middle, right = at(0), at(1), at(2)
        left = jnp.where(column == 0, left, pltpu.roll(left, 1, 1))
        right = jnp.where(column == 63, right, pltpu.roll(right, 127, 1))
        return left + middle + right

    part = [[[columns(frame_sums[f], row_tap, pair) for pair in range(2)]
             for row_tap in range(3)] for f in range(2)]

    def swap(value):
        return pltpu.roll(value, 64, 1)

    up, down = 0, 2
    halo_out[0] = jnp.where(low_half, part[0][down][0], swap(part[1][down][0]))
    halo_out[1] = jnp.where(low_half, swap(part[0][up][1]), part[1][up][1])
    halo_in[0] = jnp.where(low_half, part[0][up][0], swap(part[1][up][0]))
    halo_in[1] = jnp.where(low_half, swap(part[0][down][1]), part[1][down][1])

    pl.semaphore_wait(barrier, 15)

    to_prev = pltpu.make_async_remote_copy(
        src_ref=halo_out.at[0], dst_ref=halo_in.at[3], send_sem=halo_ssem.at[0],
        recv_sem=halo_rsem.at[0], device_id={"tile": (tile + n_tile - 1) % n_tile},
        device_id_type=MESH)
    to_next = pltpu.make_async_remote_copy(
        src_ref=halo_out.at[1], dst_ref=halo_in.at[2], send_sem=halo_ssem.at[1],
        recv_sem=halo_rsem.at[1], device_id={"tile": (tile + 1) % n_tile},
        device_id_type=MESH)
    has_prev = tile > 0
    has_next = tile < n_tile - 1

    @pl.when(has_prev)
    def _():
        to_prev.start()

    @pl.when(has_next)
    def _():
        to_next.start()

    bias_column = jnp.zeros((ZC, 128), jnp.float32)
    channel = lax.broadcasted_iota(jnp.int32, (ZC, 128), 0)
    for k in range(ZC):
        bias_column = jnp.where(channel == k, bias[k], bias_column)

    @pl.when(has_prev)
    def _():
        to_next.wait_recv()

    @pl.when(has_next)
    def _():
        to_prev.wait_recv()

    top = halo_in[jnp.where(has_prev, 2, 0)]
    bottom = halo_in[jnp.where(has_next, 3, 1)]
    latent = []
    for f in range(2):
        top_f = top if f == 0 else swap(top)
        bottom_f = swap(bottom) if f == 0 else bottom
        above = [swap(part[f][up][pair]) for pair in range(2)]
        below = [swap(part[f][down][pair]) for pair in range(2)]
        shifted_up = (jnp.where(low_half, top_f, above[0]), jnp.where(low_half, above[0], above[1]))
        shifted_down = (jnp.where(low_half, below[0], below[1]), jnp.where(low_half, below[1], bottom_f))
        for pair in range(2):
            total = shifted_up[pair] + part[f][1][pair] + shifted_down[pair] + bias_column
            latent.append(total.astype(jnp.bfloat16))

    rows_at = lax.broadcasted_iota(jnp.int32, (128, 128), 0)
    lanes_at = lax.broadcasted_iota(jnp.int32, (128, 128), 1)
    wanted_row = (lanes_at // 64) * 64 + (lanes_at % 32) * 2 + (lanes_at // 32) % 2
    selector = jnp.where(rows_at == wanted_row, 1.0, 0.0).astype(jnp.bfloat16)
    chosen = dot(jnp.concatenate(latent, axis=0), selector)
    block = lane // 32
    patch_rows = []
    for yx in range(4):
        merged = jnp.zeros((ZC, 128), jnp.float32)
        for fi in range(4):
            piece = chosen[fi * ZC : fi * ZC + ZC]
            if fi != yx:
                piece = pltpu.roll(piece, ((fi - yx) % 4) * 32, 1)
            merged = jnp.where(block == fi, piece, merged)
        patch_rows.append(merged)
    xbuf[0] = jnp.concatenate(patch_rows, axis=0).astype(jnp.bfloat16)

    x_copies = []
    for step in (4, 3, 5, 2, 6, 1, 7):
        copy = pltpu.make_async_remote_copy(
            src_ref=xbuf.at[0], dst_ref=xbuf.at[step], send_sem=x_ssem.at[step],
            recv_sem=x_rsem.at[step], device_id=at_x(step), device_id_type=MESH)
        copy.start()
        x_copies.append(copy)

    picks = []
    for at in range(4):
        first, second, count = slots[3 * at : 3 * at + 3]
        for slot, source in enumerate((first, second)):
            mine = (count > slot) & (source % 4 == hi_at * 2 + core_at)
            picks.append(jnp.where(mine, (x_at + N_X - source // 4) % N_X, N_X))

    for copy in x_copies:
        copy.wait_recv()

    for d_hi in range(2):
        for slot in range(CAP):
            pick_out[d_hi, slot] = xbuf[picks[(d_hi * 2 + 1) * 2 + slot]]
    across = pltpu.make_async_remote_copy(
        src_ref=pick_out, dst_ref=pick_in, send_sem=c_ssem.at[0], recv_sem=c_rsem.at[0],
        device_id=partner, device_id_type=MESH)
    across.start()
    own = [[xbuf[picks[d_hi * 4 + slot]] for slot in range(CAP)] for d_hi in range(2)]
    across.wait_recv()
    for d_hi in range(2):
        for slot in range(CAP):
            ysum[d_hi, slot] = own[d_hi][slot] + pick_in[d_hi, slot]

    y_copies = []
    for d_hi, d_tile in y_steps:
        at = d_hi * 4 + d_tile
        copy = pltpu.make_async_remote_copy(
            src_ref=ysum.at[d_hi], dst_ref=ybuf.at[at], send_sem=y_ssem.at[at],
            recv_sem=y_rsem.at[at], device_id=at_y(d_hi, d_tile), device_id_type=MESH)
        copy.start()
        y_copies.append(copy)
    for copy in y_copies:
        copy.wait_recv()
    for slot in range(CAP):
        for d_tile in range(4):
            own_side = ysum[0, slot] if d_tile == 0 else ybuf[d_tile, slot]
            out[slot, d_tile] = own_side + ybuf[4 + d_tile, slot]

    @pl.when(has_prev)
    def _():
        to_prev.wait_send()

    @pl.when(has_next)
    def _():
        to_next.wait_send()

    for copy in x_copies:
        copy.wait_send()
    across.wait_send()
    for copy in y_copies:
        copy.wait_send()


def route(features, taps, bias, bucket):
    return pl.pallas_call(
        route_kernel,
        out_shape=jax.ShapeDtypeStruct((CAP, 4, 64, 128), jnp.bfloat16),
        in_specs=[
            pl.BlockSpec(memory_space=pl.ANY),
            pl.BlockSpec(memory_space=pl.ANY),
            pl.BlockSpec(memory_space=pltpu.SMEM),
            pl.BlockSpec(memory_space=pltpu.SMEM),
        ],
        out_specs=pl.BlockSpec(memory_space=pltpu.VMEM),
        scratch_shapes=[
            pltpu.VMEM((2, 4, 64, 512), jnp.bfloat16),
            pltpu.VMEM((432, 512), jnp.bfloat16),
            pltpu.VMEM((2, ZC, 128), jnp.float32),
            pltpu.VMEM((4, ZC, 128), jnp.float32),
            pltpu.VMEM((N_X + 1, 64, 128), jnp.bfloat16),
            pltpu.VMEM((2, CAP, 64, 128), jnp.bfloat16),
            pltpu.VMEM((2, CAP, 64, 128), jnp.bfloat16),
            pltpu.VMEM((2, CAP, 64, 128), jnp.bfloat16),
            pltpu.VMEM((8, CAP, 64, 128), jnp.bfloat16),
            pltpu.SemaphoreType.DMA((2,)),
            pltpu.SemaphoreType.DMA((2,)),
            pltpu.SemaphoreType.DMA((2,)),
            pltpu.SemaphoreType.DMA((N_X,)),
            pltpu.SemaphoreType.DMA((N_X,)),
            pltpu.SemaphoreType.DMA((1,)),
            pltpu.SemaphoreType.DMA((1,)),
            pltpu.SemaphoreType.DMA((8,)),
            pltpu.SemaphoreType.DMA((8,)),
        ],
        compiler_params=pltpu.CompilerParams(collective_id=0, has_side_effects=True),
        name="route",
    )(features, taps, bias, bucket)


def attend_kernel(patches, weight, query_gain, key_gain, bucket, frames, out, flat, tall, ones):
    step = pl.program_id(0)
    seq = lax.axis_index("seq")
    group = lax.axis_index("group")

    def scan_slot(g, carry):
        first, second, count = carry
        hit = bucket[seq, g] == group
        total = frames[seq, g]
        first = jnp.where(hit & (count == 0), total, first)
        second = jnp.where(hit & (count == 1), total, second)
        return first, second, count + jnp.where(hit, 1, 0)

    zero = jnp.int32(0)
    slot_frames = lax.fori_loop(0, 32, scan_slot, (zero, zero, zero))[:2]

    @pl.when(step == 0)
    def _():
        token = lax.broadcasted_iota(jnp.int32, (512, 128), 0)
        for slot in range(CAP):
            valid = (token % 128) // 64 < slot_frames[slot]
            ones[slot] = jnp.where(valid, 1.0, 0.0).astype(jnp.bfloat16)
            for at in range(4):
                piece = patches[slot, at]
                flat[slot, :, at * 128 : at * 128 + 128] = piece
                upright = piece.astype(jnp.float32).T
                keep = valid[:128, :64]
                tall[0, slot, at * 128 : at * 128 + 128] = upright.astype(jnp.bfloat16)
                tall[1, slot, at * 128 : at * 128 + 128] = jnp.where(keep, upright, 0.0).astype(jnp.bfloat16)

    gain = query_gain[...] * key_gain[...] * (math.log2(math.e) / math.sqrt(HEAD))
    query_token = lax.broadcasted_iota(jnp.int32, (128, HEAD), 0)
    for slot in range(CAP):
        keep = query_token // 64 < slot_frames[slot]
        rows = tall[0, slot, :128]
        valid_rows = tall[1, slot]
        across = flat[slot]
        for local in range(PER_STEP):
            begin = local * HEAD
            head_at = pl.multiple_of(step * (PER_STEP * HEAD) + begin, HEAD)
            query_weight = weight[:, pl.ds(head_at, HEAD)]
            key_weight = weight[:, pl.ds(pl.multiple_of(head_at + D, HEAD), HEAD)]
            value_weight = weight[:, pl.ds(pl.multiple_of(head_at + 2 * D, HEAD), HEAD)]
            u = dot(rows, query_weight)
            mean = jnp.mean(u * u, axis=1, keepdims=True)
            q = (u * lax.rsqrt(mean + 1e-6) * gain).astype(jnp.bfloat16)
            u = dot(key_weight, across, ((0,), (0,)))
            mean = jnp.mean(u * u, axis=0, keepdims=True)
            k = (u * lax.rsqrt(mean + 1e-6)).astype(jnp.bfloat16)
            v = dot(valid_rows, value_weight).astype(jnp.bfloat16)
            weights = jnp.exp2(dot(q, k)).astype(jnp.bfloat16)
            mixed = dot(weights, jnp.concatenate([v, ones[slot]], axis=1))
            result = mixed[:, :HEAD] / mixed[:, HEAD:]
            out[0, 0, slot, :, begin : begin + HEAD] = jnp.where(keep, result, 0.0).astype(jnp.bfloat16)


def attend(patches, weight, query_gain, key_gain, bucket, frames):
    whole = pl.BlockSpec(memory_space=pltpu.VMEM)
    return pl.pallas_call(
        attend_kernel,
        grid=(STEPS,),
        out_shape=jax.ShapeDtypeStruct((1, 1, CAP, 128, D), jnp.bfloat16),
        in_specs=[
            whole, whole, whole, whole,
            pl.BlockSpec(memory_space=pltpu.SMEM),
            pl.BlockSpec(memory_space=pltpu.SMEM),
        ],
        out_specs=pl.BlockSpec((1, 1, CAP, 128, PER_STEP * HEAD), lambda i: (0, 0, 0, 0, i)),
        scratch_shapes=[
            pltpu.VMEM((CAP, 64, 512), jnp.bfloat16),
            pltpu.VMEM((2, CAP, 512, 64), jnp.bfloat16),
            pltpu.VMEM((CAP, 512, 128), jnp.bfloat16),
        ],
        name="attend",
    )(patches, weight, query_gain, key_gain, bucket, frames)


def shards(features, conv_weight, conv_bias, embed_qkv, query_gain, key_gain, bucket, frames):
    taps = jnp.transpose(conv_weight, (0, 1, 2, 4, 3)).reshape(432, 512)
    patches = route(features[0, 0], taps, conv_bias, bucket)
    return attend(
        patches, embed_qkv, query_gain.reshape(1, HEAD), key_gain.reshape(1, HEAD), bucket, frames
    )


def solution(mesh):
    in_specs = (P("seq", "group", None, "tile", None, None), P(), P(), P(), P(), P(), P(), P())
    out_specs = P("seq", "group", None, "tile", None)
    return jax.shard_map(shards, mesh=mesh, in_specs=in_specs, out_specs=out_specs, check_vma=False)
```

```python
import math

import jax
import jax.numpy as jnp
from jax import lax
from jax.experimental import pallas as pl
from jax.experimental.pallas import tpu as pltpu
from jax.sharding import PartitionSpec as P

HEADS = 12
HEAD = 128
D = 1536
CAP = 2
N_X = 8
ZC = 16
MESH = pl.DeviceIdType.MESH


def dot(a, b, dims=((1,), (0,))):
    return lax.dot_general(a, b, (dims, ((), ())), preferred_element_type=jnp.float32)


def fused_kernel(feat_hbm, taps_hbm, bias_hbm, embed_hbm, query_gain, key_gain, bucket_hbm,
                 frames_hbm, out_hbm,
                 feat, taps_ref, bias, embed, bucket, frames, key_rows, halo_out, halo_in,
                 xbuf, pick_out, pick_in, ysum, ybuf, queries, keys, values, ones, soft, result,
                 load_sem, halo_ssem, halo_rsem, x_ssem, x_rsem, c_ssem, c_rsem, y_ssem, y_rsem,
                 out_sem):
    tile = lax.axis_index("tile")
    seq = lax.axis_index("seq")
    group = lax.axis_index("group")
    n_tile = lax.axis_size("tile")
    x_at = group // 4
    hi_at = (group // 2) % 2
    core_at = group % 2

    def at_x(step):
        return {"group": ((x_at + step) % N_X) * 4 + hi_at * 2 + core_at}

    def at_y(step_hi, step_tile):
        return {"tile": (tile + step_tile) % n_tile,
                "group": x_at * 4 + ((hi_at + step_hi) % 2) * 2 + core_at}

    partner = {"group": x_at * 4 + hi_at * 2 + (1 - core_at)}
    y_steps = [(1, 0), (1, 1), (1, 3), (1, 2), (0, 2), (0, 1), (0, 3)]

    loads = [
        pltpu.make_async_copy(source, target, load_sem.at[at])
        for at, (source, target) in enumerate((
            (taps_hbm, taps_ref), (feat_hbm, feat), (bias_hbm, bias), (bucket_hbm, bucket),
            (frames_hbm, frames), (embed_hbm, embed)))
    ]
    for load in loads:
        load.start()

    barrier = pltpu.get_barrier_semaphore()
    for step in (4, 3, 5, 2, 6, 1, 7):
        pl.semaphore_signal(barrier, inc=1, device_id=at_x(step), device_id_type=MESH)
    for step in y_steps:
        pl.semaphore_signal(barrier, inc=1, device_id=at_y(*step), device_id_type=MESH)
    pl.semaphore_signal(barrier, inc=1, device_id=partner, device_id_type=MESH)

    xbuf[N_X] = jnp.zeros((64, 128), jnp.bfloat16)
    for load in loads[:2]:
        load.wait()
    taps = taps_ref[...]
    first_frame = feat[0].reshape(256, 512)
    second_frame = feat[1].reshape(256, 512)
    from_first = dot(taps, first_frame, ((1,), (1,)))
    from_second = dot(taps[288:], second_frame, ((1,), (1,)))
    both = from_first[:144] + from_first[144:288]
    frame_sums = (both + from_first[288:], both + from_second)

    lane = lax.broadcasted_iota(jnp.int32, (ZC, 128), 1)
    column = lane % 64
    low_half = lane < 64

    def columns(sums, row_tap, pair):
        def at(col_tap):
            begin = (row_tap * 3 + col_tap) * ZC
            return sums[begin : begin + ZC, pair * 128 : pair * 128 + 128]

        left, middle, right = at(0), at(1), at(2)
        left = jnp.where(column == 0, left, pltpu.roll(left, 1, 1))
        right = jnp.where(column == 63, right, pltpu.roll(right, 127, 1))
        return left + middle + right

    part = [[[columns(frame_sums[f], row_tap, pair) for pair in range(2)]
             for row_tap in range(3)] for f in range(2)]

    def swap(value):
        return pltpu.roll(value, 64, 1)

    up, down = 0, 2
    halo_out[0] = jnp.where(low_half, part[0][down][0], swap(part[1][down][0]))
    halo_out[1] = jnp.where(low_half, swap(part[0][up][1]), part[1][up][1])
    halo_in[0] = jnp.where(low_half, part[0][up][0], swap(part[1][up][0]))
    halo_in[1] = jnp.where(low_half, swap(part[0][down][1]), part[1][down][1])

    pl.semaphore_wait(barrier, 15)

    to_prev = pltpu.make_async_remote_copy(
        src_ref=halo_out.at[0], dst_ref=halo_in.at[3], send_sem=halo_ssem.at[0],
        recv_sem=halo_rsem.at[0], device_id={"tile": (tile + n_tile - 1) % n_tile},
        device_id_type=MESH)
    to_next = pltpu.make_async_remote_copy(
        src_ref=halo_out.at[1], dst_ref=halo_in.at[2], send_sem=halo_ssem.at[1],
        recv_sem=halo_rsem.at[1], device_id={"tile": (tile + 1) % n_tile},
        device_id_type=MESH)
    has_prev = tile > 0
    has_next = tile < n_tile - 1

    @pl.when(has_prev)
    def _():
        to_prev.start()

    @pl.when(has_next)
    def _():
        to_next.start()

    for load in loads[2:5]:
        load.wait()
    buckets = [x_at * 4 + ((hi_at + d_hi) % 2) * 2 + (core_at + d_core) % 2
               for d_hi in range(2) for d_core in range(2)]

    def scan_slot(g, carry):
        here = bucket[seq, g]
        done = []
        for at, wanted in enumerate(buckets):
            first, second, count = carry[3 * at : 3 * at + 3]
            hit = here == wanted
            first = jnp.where(hit & (count == 0), g, first)
            second = jnp.where(hit & (count == 1), g, second)
            count = count + jnp.where(hit, 1, 0)
            done += [first, second, count]
        return tuple(done)

    slots = lax.fori_loop(0, 32, scan_slot, (jnp.int32(0),) * 12)

    bias_column = jnp.zeros((ZC, 128), jnp.float32)
    channel = lax.broadcasted_iota(jnp.int32, (ZC, 128), 0)
    for k in range(ZC):
        bias_column = jnp.where(channel == k, bias[k], bias_column)

    @pl.when(has_prev)
    def _():
        to_next.wait_recv()

    @pl.when(has_next)
    def _():
        to_prev.wait_recv()

    top = halo_in[jnp.where(has_prev, 2, 0)]
    bottom = halo_in[jnp.where(has_next, 3, 1)]
    latent = []
    for f in range(2):
        top_f = top if f == 0 else swap(top)
        bottom_f = swap(bottom) if f == 0 else bottom
        above = [swap(part[f][up][pair]) for pair in range(2)]
        below = [swap(part[f][down][pair]) for pair in range(2)]
        shifted_up = (jnp.where(low_half, top_f, above[0]), jnp.where(low_half, above[0], above[1]))
        shifted_down = (jnp.where(low_half, below[0], below[1]), jnp.where(low_half, below[1], bottom_f))
        for pair in range(2):
            total = shifted_up[pair] + part[f][1][pair] + shifted_down[pair] + bias_column
            latent.append(total.astype(jnp.bfloat16))

    rows_at = lax.broadcasted_iota(jnp.int32, (128, 128), 0)
    lanes_at = lax.broadcasted_iota(jnp.int32, (128, 128), 1)
    wanted_row = (lanes_at // 64) * 64 + (lanes_at % 32) * 2 + (lanes_at // 32) % 2
    selector = jnp.where(rows_at == wanted_row, 1.0, 0.0).astype(jnp.bfloat16)
    chosen = dot(jnp.concatenate(latent, axis=0), selector)
    block = lane // 32
    patch_rows = []
    for yx in range(4):
        merged = jnp.zeros((ZC, 128), jnp.float32)
        for fi in range(4):
            piece = chosen[fi * ZC : fi * ZC + ZC]
            if fi != yx:
                piece = pltpu.roll(piece, ((fi - yx) % 4) * 32, 1)
            merged = jnp.where(block == fi, piece, merged)
        patch_rows.append(merged)
    xbuf[0] = jnp.concatenate(patch_rows, axis=0).astype(jnp.bfloat16)

    x_copies = []
    for step in (4, 3, 5, 2, 6, 1, 7):
        copy = pltpu.make_async_remote_copy(
            src_ref=xbuf.at[0], dst_ref=xbuf.at[step], send_sem=x_ssem.at[step],
            recv_sem=x_rsem.at[step], device_id=at_x(step), device_id_type=MESH)
        copy.start()
        x_copies.append(copy)

    picks = []
    for at in range(4):
        first, second, count = slots[3 * at : 3 * at + 3]
        for slot, source in enumerate((first, second)):
            mine = (count > slot) & (source % 4 == hi_at * 2 + core_at)
            picks.append(jnp.where(mine, (x_at + N_X - source // 4) % N_X, N_X))

    loads[5].wait()
    for at in range(HEADS):
        piece = embed[:, D + at * HEAD : D + at * HEAD + HEAD]
        key_rows[at * HEAD : at * HEAD + HEAD] = piece.astype(jnp.float32).T.astype(jnp.bfloat16)
    gain = query_gain[...] * key_gain[...] * (math.log2(math.e) / math.sqrt(HEAD))
    token = lax.broadcasted_iota(jnp.int32, (128, HEAD), 0)
    valid = []
    for slot in range(CAP):
        first, second, count = slots[:3]
        total = jnp.where(count > slot, frames[seq, second if slot else first], 0)
        keep = token // 64 < total
        valid.append(keep)
        ones[slot] = jnp.where(keep, 1.0, 0.0).astype(jnp.bfloat16)

    for copy in x_copies:
        copy.wait_recv()

    for d_hi in range(2):
        for slot in range(CAP):
            pick_out[d_hi, slot] = xbuf[picks[(d_hi * 2 + 1) * 2 + slot]]
    across = pltpu.make_async_remote_copy(
        src_ref=pick_out, dst_ref=pick_in, send_sem=c_ssem.at[0], recv_sem=c_rsem.at[0],
        device_id=partner, device_id_type=MESH)
    across.start()
    own = [[xbuf[picks[d_hi * 4 + slot]] for slot in range(CAP)] for d_hi in range(2)]
    across.wait_recv()
    for d_hi in range(2):
        for slot in range(CAP):
            ysum[d_hi, slot] = own[d_hi][slot] + pick_in[d_hi, slot]

    y_copies = []
    for d_hi, d_tile in y_steps:
        at = d_hi * 4 + d_tile
        copy = pltpu.make_async_remote_copy(
            src_ref=ysum.at[d_hi], dst_ref=ybuf.at[at], send_sem=y_ssem.at[at],
            recv_sem=y_rsem.at[at], device_id=at_y(d_hi, d_tile), device_id_type=MESH)
        copy.start()
        y_copies.append(copy)
    arrivals = {step: copy for step, copy in zip(y_steps, y_copies)}
    for d_tile in range(4):
        arrivals[1, d_tile].wait_recv()
        if d_tile:
            arrivals[0, d_tile].wait_recv()
        near = ysum if d_tile == 0 else ybuf
        parts = [near[d_tile, slot] + ybuf[4 + d_tile, slot] for slot in range(CAP)]
        upright = [parts[slot].astype(jnp.float32).T for slot in range(CAP)]
        if d_tile == 0:
            for slot in range(CAP):
                u = dot(upright[slot].astype(jnp.bfloat16), embed[:, :D])
                for at in range(HEADS):
                    mine = u[:, at * HEAD : at * HEAD + HEAD]
                    mean = jnp.mean(mine * mine, axis=1, keepdims=True)
                    queries[slot, at] = (mine * lax.rsqrt(mean + 1e-6) * gain).astype(jnp.bfloat16)
        joined = jnp.concatenate(parts, axis=1)
        for at in range(HEADS):
            u = dot(key_rows[at * HEAD : at * HEAD + HEAD], joined)
            mean = jnp.mean(u * u, axis=0, keepdims=True)
            keys[d_tile, at] = (u * lax.rsqrt(mean + 1e-6)).astype(jnp.bfloat16)
        tall = jnp.concatenate(
            [jnp.where(valid[slot][:, :64], upright[slot], 0.0) for slot in range(CAP)], axis=0
        ).astype(jnp.bfloat16)
        for at in range(0, HEADS, 2):
            begin = 2 * D + at * HEAD
            v = dot(tall, embed[:, begin : begin + 2 * HEAD]).astype(jnp.bfloat16)
            values[d_tile, at] = v[:, :HEAD]
            values[d_tile, at + 1] = v[:, HEAD:]

    units = [(at, slot) for at in range(HEADS) for slot in range(CAP)]
    out_copies = []
    for turn in range(len(units) + 1):
        if turn < len(units):
            at, slot = units[turn]
            begin = slot * HEAD
            k = jnp.concatenate(
                [keys[part, at, :, begin : begin + HEAD] for part in range(4)], axis=1)
            soft[turn % 3] = jnp.exp2(dot(queries[slot, at], k)).astype(jnp.bfloat16)
        if turn:
            at, slot = units[turn - 1]
            begin = slot * HEAD
            v = jnp.concatenate(
                [jnp.concatenate([values[part, at, begin : begin + HEAD], ones[slot]], axis=1)
                 for part in range(4)], axis=0)
            mixed = dot(soft[(turn - 1) % 3], v)
            final = jnp.where(valid[slot], mixed[:, :HEAD] / mixed[:, HEAD:], 0.0)
            result[slot, :, at * HEAD : at * HEAD + HEAD] = final.astype(jnp.bfloat16)
            if slot == CAP - 1 and at % 3 == 2:
                spot = pl.ds((at - 2) * HEAD, 3 * HEAD)
                copy = pltpu.make_async_copy(
                    result.at[:, :, spot], out_hbm.at[0, 0, :, :, spot], out_sem.at[at // 3])
                copy.start()
                out_copies.append(copy)
    for copy in out_copies:
        copy.wait()

    @pl.when(has_prev)
    def _():
        to_prev.wait_send()

    @pl.when(has_next)
    def _():
        to_next.wait_send()

    for copy in x_copies:
        copy.wait_send()
    across.wait_send()
    for copy in y_copies:
        copy.wait_send()


def fused(features, taps, bias, embed, query_gain, key_gain, bucket, frames):
    anywhere = pl.BlockSpec(memory_space=pl.ANY)
    vector = pl.BlockSpec(memory_space=pltpu.VMEM)
    return pl.pallas_call(
        fused_kernel,
        out_shape=jax.ShapeDtypeStruct((1, 1, CAP, 128, D), jnp.bfloat16),
        in_specs=[anywhere, anywhere, anywhere, anywhere, vector, vector, anywhere, anywhere],
        out_specs=anywhere,
        scratch_shapes=[
            pltpu.VMEM((2, 4, 64, 512), jnp.bfloat16),
            pltpu.VMEM((432, 512), jnp.bfloat16),
            pltpu.SMEM((ZC,), jnp.float32),
            pltpu.VMEM((64, 3 * D), jnp.bfloat16),
            pltpu.SMEM((8, 32), jnp.int32),
            pltpu.SMEM((8, 32), jnp.int32),
            pltpu.VMEM((D, 64), jnp.bfloat16),
            pltpu.VMEM((2, ZC, 128), jnp.float32),
            pltpu.VMEM((4, ZC, 128), jnp.float32),
            pltpu.VMEM((N_X + 1, 64, 128), jnp.bfloat16),
            pltpu.VMEM((2, CAP, 64, 128), jnp.bfloat16),
            pltpu.VMEM((2, CAP, 64, 128), jnp.bfloat16),
            pltpu.VMEM((2, CAP, 64, 128), jnp.bfloat16),
            pltpu.VMEM((8, CAP, 64, 128), jnp.bfloat16),
            pltpu.VMEM((CAP, HEADS, 128, HEAD), jnp.bfloat16),
            pltpu.VMEM((4, HEADS, HEAD, CAP * 128), jnp.bfloat16),
            pltpu.VMEM((4, HEADS, CAP * 128, HEAD), jnp.bfloat16),
            pltpu.VMEM((CAP, 128, HEAD), jnp.bfloat16),
            pltpu.VMEM((3, 128, 512), jnp.bfloat16),
            pltpu.VMEM((CAP, 128, D), jnp.bfloat16),
            pltpu.SemaphoreType.DMA((6,)),
            pltpu.SemaphoreType.DMA((2,)),
            pltpu.SemaphoreType.DMA((2,)),
            pltpu.SemaphoreType.DMA((N_X,)),
            pltpu.SemaphoreType.DMA((N_X,)),
            pltpu.SemaphoreType.DMA((1,)),
            pltpu.SemaphoreType.DMA((1,)),
            pltpu.SemaphoreType.DMA((8,)),
            pltpu.SemaphoreType.DMA((8,)),
            pltpu.SemaphoreType.DMA((4,)),
        ],
        compiler_params=pltpu.CompilerParams(collective_id=0, has_side_effects=True),
        name="fused",
    )(features, taps, bias, embed, query_gain, key_gain, bucket, frames)


def shards(features, conv_weight, conv_bias, embed_qkv, query_gain, key_gain, bucket, frames):
    taps = jnp.transpose(conv_weight, (0, 1, 2, 4, 3)).reshape(432, 512)
    return fused(
        features[0, 0], taps, conv_bias, embed_qkv, query_gain.reshape(1, HEAD),
        key_gain.reshape(1, HEAD), bucket, frames
    )


def solution(mesh):
    in_specs = (P("seq", "group", None, "tile", None, None), P(), P(), P(), P(), P(), P(), P())
    out_specs = P("seq", "group", None, "tile", None)
    return jax.shard_map(shards, mesh=mesh, in_specs=in_specs, out_specs=out_specs, check_vma=False)
```

```python
import functools
import math

import jax
import jax.numpy as jnp
from jax import lax
from jax.experimental import pallas as pl
from jax.experimental.pallas import tpu as pltpu
from jax.sharding import PartitionSpec as P

HEADS = 12
HEAD = 128
D = 1536
CAP = 2
N_X = 8
ZC = 16
MESH = pl.DeviceIdType.MESH


def dot(a, b, dims=((1,), (0,))):
    return lax.dot_general(a, b, (dims, ((), ())), preferred_element_type=jnp.float32)


def fused_kernel(feat_hbm, taps_hbm, bias_hbm, embed_hbm, query_gain, key_gain, bucket_hbm,
                 frames_hbm, result,
                 feat, taps_ref, bias, embed, gains, bucket, frames, key_rows, halo_out, halo_in,
                 xbuf, pick_out, pick_in, ysum, ybuf, part_now, queries, keys, values, ones, soft,
                 load_sem, halo_ssem, halo_rsem, x_ssem, x_rsem, c_ssem, c_rsem, y_ssem, y_rsem):
    tile = lax.axis_index("tile")
    seq = lax.axis_index("seq")
    group = lax.axis_index("group")
    n_tile = lax.axis_size("tile")
    x_at = group // 4
    hi_at = (group // 2) % 2
    core_at = group % 2

    def at_x(step):
        return {"group": ((x_at + step) % N_X) * 4 + hi_at * 2 + core_at}

    def at_y(step_hi, step_tile):
        return {"tile": (tile + step_tile) % n_tile,
                "group": x_at * 4 + ((hi_at + step_hi) % 2) * 2 + core_at}

    partner = {"group": x_at * 4 + hi_at * 2 + (1 - core_at)}
    x_steps = (4, 3, 5, 2, 6, 1, 7)
    y_steps = [(1, 0), (1, 1), (1, 3), (1, 2), (0, 2), (0, 1), (0, 3)]

    loads = [
        pltpu.make_async_copy(source, target, load_sem.at[at])
        for at, (source, target) in enumerate((
            (taps_hbm, taps_ref), (feat_hbm, feat), (bias_hbm, bias), (bucket_hbm, bucket),
            (frames_hbm, frames), (embed_hbm, embed), (query_gain, gains.at[0]),
            (key_gain, gains.at[1])))
    ]
    for load in loads:
        load.start()
    barrier = pltpu.get_barrier_semaphore()
    for step in x_steps:
        pl.semaphore_signal(barrier, inc=1, device_id=at_x(step), device_id_type=MESH)
    for step in y_steps:
        pl.semaphore_signal(barrier, inc=1, device_id=at_y(*step), device_id_type=MESH)
    pl.semaphore_signal(barrier, inc=1, device_id=partner, device_id_type=MESH)
    xbuf[N_X] = jnp.zeros((64, 128), jnp.bfloat16)
    for load in loads[:2]:
        load.wait()
    taps = taps_ref[...]
    first_frame = feat[0].reshape(256, 512)
    second_frame = feat[1].reshape(256, 512)
    from_first = dot(taps, first_frame, ((1,), (1,)))
    from_second = dot(taps[288:], second_frame, ((1,), (1,)))
    both = from_first[:144] + from_first[144:288]
    frame_sums = (both + from_first[288:], both + from_second)

    lane = lax.broadcasted_iota(jnp.int32, (ZC, 128), 1)
    column = lane % 64
    low_half = lane < 64

    def columns(sums, row_tap, pair):
        def at(col_tap):
            begin = (row_tap * 3 + col_tap) * ZC
            return sums[begin : begin + ZC, pair * 128 : pair * 128 + 128]

        left, middle, right = at(0), at(1), at(2)
        left = jnp.where(column == 0, left, pltpu.roll(left, 1, 1))
        right = jnp.where(column == 63, right, pltpu.roll(right, 127, 1))
        return left + middle + right

    part = [[[columns(frame_sums[f], row_tap, pair) for pair in range(2)]
             for row_tap in range(3)] for f in range(2)]

    def swap(value):
        return pltpu.roll(value, 64, 1)

    up, down = 0, 2
    halo_out[0] = jnp.where(low_half, part[0][down][0], swap(part[1][down][0]))
    halo_out[1] = jnp.where(low_half, swap(part[0][up][1]), part[1][up][1])
    halo_in[0] = jnp.where(low_half, part[0][up][0], swap(part[1][up][0]))
    halo_in[1] = jnp.where(low_half, swap(part[0][down][1]), part[1][down][1])

    pl.semaphore_wait(barrier, 15)

    to_prev = pltpu.make_async_remote_copy(
        src_ref=halo_out.at[0], dst_ref=halo_in.at[3], send_sem=halo_ssem.at[0],
        recv_sem=halo_rsem.at[0], device_id={"tile": (tile + n_tile - 1) % n_tile},
        device_id_type=MESH)
    to_next = pltpu.make_async_remote_copy(
        src_ref=halo_out.at[1], dst_ref=halo_in.at[2], send_sem=halo_ssem.at[1],
        recv_sem=halo_rsem.at[1], device_id={"tile": (tile + 1) % n_tile},
        device_id_type=MESH)
    has_prev = tile > 0
    has_next = tile < n_tile - 1

    @pl.when(has_prev)
    def _():
        to_prev.start()

    @pl.when(has_next)
    def _():
        to_next.start()

    for load in loads[2:5]:
        load.wait()
    buckets = [x_at * 4 + ((hi_at + d_hi) % 2) * 2 + (core_at + d_core) % 2
               for d_hi in range(2) for d_core in range(2)]

    def scan_slot(g, carry):
        here = bucket[seq, g]
        done = []
        for at, wanted in enumerate(buckets):
            first, second, count = carry[3 * at : 3 * at + 3]
            hit = here == wanted
            first = jnp.where(hit & (count == 0), g, first)
            second = jnp.where(hit & (count == 1), g, second)
            count = count + jnp.where(hit, 1, 0)
            done += [first, second, count]
        return tuple(done)

    slots = lax.fori_loop(0, 32, scan_slot, (jnp.int32(0),) * 12)

    bias_column = jnp.zeros((ZC, 128), jnp.float32)
    channel = lax.broadcasted_iota(jnp.int32, (ZC, 128), 0)
    for k in range(ZC):
        bias_column = jnp.where(channel == k, bias[k], bias_column)

    @pl.when(has_prev)
    def _():
        to_next.wait_recv()

    @pl.when(has_next)
    def _():
        to_prev.wait_recv()

    top = halo_in[jnp.where(has_prev, 2, 0)]
    bottom = halo_in[jnp.where(has_next, 3, 1)]
    latent = []
    for f in range(2):
        top_f = top if f == 0 else swap(top)
        bottom_f = swap(bottom) if f == 0 else bottom
        above = [swap(part[f][up][pair]) for pair in range(2)]
        below = [swap(part[f][down][pair]) for pair in range(2)]
        shifted_up = (jnp.where(low_half, top_f, above[0]), jnp.where(low_half, above[0], above[1]))
        shifted_down = (jnp.where(low_half, below[0], below[1]), jnp.where(low_half, below[1], bottom_f))
        for pair in range(2):
            total = shifted_up[pair] + part[f][1][pair] + shifted_down[pair] + bias_column
            latent.append(total.astype(jnp.bfloat16))

    rows_at = lax.broadcasted_iota(jnp.int32, (128, 128), 0)
    lanes_at = lax.broadcasted_iota(jnp.int32, (128, 128), 1)
    wanted_row = (lanes_at // 64) * 64 + (lanes_at % 32) * 2 + (lanes_at // 32) % 2
    selector = jnp.where(rows_at == wanted_row, 1.0, 0.0).astype(jnp.bfloat16)
    chosen = dot(jnp.concatenate(latent, axis=0), selector)
    block = lane // 32
    patch_rows = []
    for yx in range(4):
        merged = jnp.zeros((ZC, 128), jnp.float32)
        for fi in range(4):
            piece = chosen[fi * ZC : fi * ZC + ZC]
            if fi != yx:
                piece = pltpu.roll(piece, ((fi - yx) % 4) * 32, 1)
            merged = jnp.where(block == fi, piece, merged)
        patch_rows.append(merged)
    xbuf[0] = jnp.concatenate(patch_rows, axis=0).astype(jnp.bfloat16)

    x_copies = []
    for step in (4, 3, 5, 2, 6, 1, 7):
        copy = pltpu.make_async_remote_copy(
            src_ref=xbuf.at[0], dst_ref=xbuf.at[step], send_sem=x_ssem.at[step],
            recv_sem=x_rsem.at[step], device_id=at_x(step), device_id_type=MESH)
        copy.start()
        x_copies.append(copy)

    picks = []
    for at in range(4):
        first, second, count = slots[3 * at : 3 * at + 3]
        for slot, source in enumerate((first, second)):
            mine = (count > slot) & (source % 4 == hi_at * 2 + core_at)
            picks.append(jnp.where(mine, (x_at + N_X - source // 4) % N_X, N_X))

    for load in loads[5:]:
        load.wait()
    for at in range(HEADS):
        piece = embed[:, D + at * HEAD : D + at * HEAD + HEAD]
        key_rows[at * HEAD : at * HEAD + HEAD] = piece.astype(jnp.float32).T.astype(jnp.bfloat16)
    gain = gains[0] * gains[1] * (math.log2(math.e) / math.sqrt(HEAD))
    token = lax.broadcasted_iota(jnp.int32, (128, HEAD), 0)
    valid = []
    for slot in range(CAP):
        first, second, count = slots[:3]
        total = jnp.where(count > slot, frames[seq, second if slot else first], 0)
        keep = token // 64 < total
        valid.append(keep)
        ones[slot] = jnp.where(keep, 1.0, 0.0).astype(jnp.bfloat16)

    for copy in x_copies:
        copy.wait_recv()

    for d_hi in range(2):
        for slot in range(CAP):
            pick_out[d_hi, slot] = xbuf[picks[(d_hi * 2 + 1) * 2 + slot]]
    across = pltpu.make_async_remote_copy(
        src_ref=pick_out, dst_ref=pick_in, send_sem=c_ssem.at[0], recv_sem=c_rsem.at[0],
        device_id=partner, device_id_type=MESH)
    across.start()
    own = [[xbuf[picks[d_hi * 4 + slot]] for slot in range(CAP)] for d_hi in range(2)]
    across.wait_recv()
    for d_hi in range(2):
        for slot in range(CAP):
            ysum[d_hi, slot] = own[d_hi][slot] + pick_in[d_hi, slot]

    y_copies = []
    for d_hi, d_tile in y_steps:
        at = d_hi * 4 + d_tile
        copy = pltpu.make_async_remote_copy(
            src_ref=ysum.at[d_hi], dst_ref=ybuf.at[at], send_sem=y_ssem.at[at],
            recv_sem=y_rsem.at[at], device_id=at_y(d_hi, d_tile), device_id_type=MESH)
        copy.start()
        y_copies.append(copy)
    arrivals = {step: copy for step, copy in zip(y_steps, y_copies)}
    turns = ((2, 3, 0, 1), (2, 3, 1, 0), (2, 3, 0, 1), (2, 3, 0, 1))

    def take(d_tile):
        arrivals[1, d_tile].wait_recv()
        if d_tile:
            arrivals[0, d_tile].wait_recv()
        near = ybuf if d_tile else ysum
        for slot in range(CAP):
            part_now[slot] = near[d_tile, slot] + ybuf[4 + d_tile, slot]

    def make_queries():
        for slot in range(CAP):
            u = dot(part_now[slot].astype(jnp.float32).T.astype(jnp.bfloat16), embed[:, :D])
            for at in range(HEADS):
                mine = u[:, at * HEAD : at * HEAD + HEAD]
                mean = jnp.mean(mine * mine, axis=1, keepdims=True)
                queries[slot, at] = (mine * lax.rsqrt(mean + 1e-6) * gain).astype(jnp.bfloat16)

    for turn in range(4):
        for here in range(4):
            pl.when(tile == here)(functools.partial(take, (here - turns[here][turn]) % 4))
        own_turn = {0: tile == 2, 1: tile == 3, 2: tile < 2}
        if turn in own_turn:
            pl.when(own_turn[turn])(make_queries)
        parts = [part_now[slot] for slot in range(CAP)]
        joined = jnp.concatenate(parts, axis=1)
        for at in range(HEADS):
            u = dot(key_rows[at * HEAD : at * HEAD + HEAD], joined)
            mean = jnp.mean(u * u, axis=0, keepdims=True)
            keys[turn, at] = (u * lax.rsqrt(mean + 1e-6)).astype(jnp.bfloat16)
        tall = jnp.concatenate(
            [jnp.where(valid[slot][:, :64], parts[slot].astype(jnp.float32).T, 0.0)
             for slot in range(CAP)], axis=0
        ).astype(jnp.bfloat16)
        for at in range(0, HEADS, 2):
            begin = 2 * D + at * HEAD
            v = dot(tall, embed[:, begin : begin + 2 * HEAD]).astype(jnp.bfloat16)
            values[turn, at] = v[:, :HEAD]
            values[turn, at + 1] = v[:, HEAD:]

    units = [(at, slot) for at in range(HEADS) for slot in range(CAP)]
    for turn in range(len(units) + 1):
        if turn < len(units):
            at, slot = units[turn]
            begin = slot * HEAD
            k = jnp.concatenate(
                [keys[part, at, :, begin : begin + HEAD] for part in range(4)], axis=1)
            soft[turn % 3] = jnp.exp2(dot(queries[slot, at], k)).astype(jnp.bfloat16)
        if turn:
            at, slot = units[turn - 1]
            begin = slot * HEAD
            v = jnp.concatenate(
                [jnp.concatenate([values[part, at, begin : begin + HEAD], ones[slot]], axis=1)
                 for part in range(4)], axis=0)
            mixed = dot(soft[(turn - 1) % 3], v)
            final = jnp.where(valid[slot], mixed[:, :HEAD] / mixed[:, HEAD:], 0.0)
            result[0, 0, slot, :, at * HEAD : at * HEAD + HEAD] = final.astype(jnp.bfloat16)

    @pl.when(has_prev)
    def _():
        to_prev.wait_send()

    @pl.when(has_next)
    def _():
        to_next.wait_send()

    for copy in x_copies:
        copy.wait_send()
    across.wait_send()
    for copy in y_copies:
        copy.wait_send()


def fused(features, taps, bias, embed, query_gain, key_gain, bucket, frames):
    anywhere = pl.BlockSpec(memory_space=pltpu.HBM)
    vector = pl.BlockSpec(memory_space=pltpu.VMEM)
    return pl.pallas_call(
        fused_kernel,
        out_shape=pltpu.VMEM((1, 1, CAP, 128, D), jnp.bfloat16),
        in_specs=[anywhere] * 8,
        out_specs=vector,
        scratch_shapes=[
            pltpu.VMEM((2, 4, 64, 512), jnp.bfloat16),
            pltpu.VMEM((432, 512), jnp.bfloat16),
            pltpu.SMEM((ZC,), jnp.float32),
            pltpu.VMEM((64, 3 * D), jnp.bfloat16),
            pltpu.VMEM((2, 1, HEAD), jnp.float32),
            pltpu.SMEM((8, 32), jnp.int32),
            pltpu.SMEM((8, 32), jnp.int32),
            pltpu.VMEM((D, 64), jnp.bfloat16),
            pltpu.VMEM((2, ZC, 128), jnp.float32),
            pltpu.VMEM((4, ZC, 128), jnp.float32),
            pltpu.VMEM((N_X + 1, 64, 128), jnp.bfloat16),
            pltpu.VMEM((2, CAP, 64, 128), jnp.bfloat16),
            pltpu.VMEM((2, CAP, 64, 128), jnp.bfloat16),
            pltpu.VMEM((2, CAP, 64, 128), jnp.bfloat16),
            pltpu.VMEM((8, CAP, 64, 128), jnp.bfloat16),
            pltpu.VMEM((CAP, 64, 128), jnp.bfloat16),
            pltpu.VMEM((CAP, HEADS, 128, HEAD), jnp.bfloat16),
            pltpu.VMEM((4, HEADS, HEAD, CAP * 128), jnp.bfloat16),
            pltpu.VMEM((4, HEADS, CAP * 128, HEAD), jnp.bfloat16),
            pltpu.VMEM((CAP, 128, HEAD), jnp.bfloat16),
            pltpu.VMEM((3, 128, 512), jnp.bfloat16),
            pltpu.SemaphoreType.DMA((8,)),
            pltpu.SemaphoreType.DMA((2,)),
            pltpu.SemaphoreType.DMA((2,)),
            pltpu.SemaphoreType.DMA((N_X,)),
            pltpu.SemaphoreType.DMA((N_X,)),
            pltpu.SemaphoreType.DMA((1,)),
            pltpu.SemaphoreType.DMA((1,)),
            pltpu.SemaphoreType.DMA((8,)),
            pltpu.SemaphoreType.DMA((8,)),
        ],
        compiler_params=pltpu.CompilerParams(
            collective_id=0, has_side_effects=True, vmem_limit_bytes=40 * 2**20),
        name="fused",
    )(*(pltpu.with_memory_space_constraint(array, pltpu.HBM) for array in (
        features, taps, bias, embed, query_gain, key_gain, bucket, frames)))


def shards(features, conv_weight, conv_bias, embed_qkv, query_gain, key_gain, bucket, frames):
    taps = jnp.transpose(conv_weight, (0, 1, 2, 4, 3)).reshape(432, 512)
    return fused(
        features[0, 0], taps, conv_bias, embed_qkv, query_gain.reshape(1, HEAD),
        key_gain.reshape(1, HEAD), bucket, frames
    )


def solution(mesh):
    in_specs = (P("seq", "group", None, "tile", None, None), P(), P(), P(), P(), P(), P(), P())
    out_specs = P("seq", "group", None, "tile", None)
    return jax.shard_map(shards, mesh=mesh, in_specs=in_specs, out_specs=out_specs, check_vma=False)
```

```python
import functools
import math

import jax
import jax.numpy as jnp
from jax import lax
from jax.experimental import pallas as pl
from jax.experimental.pallas import tpu as pltpu
from jax.sharding import PartitionSpec as P

HEADS = 12
HEAD = 128
D = 1536
CAP = 2
N_X = 8
ZC = 16
MESH = pl.DeviceIdType.MESH


def dot(a, b, dims=((1,), (0,))):
    return lax.dot_general(a, b, (dims, ((), ())), preferred_element_type=jnp.float32)


def fused_kernel(feat_hbm, taps_hbm, bias_hbm, embed_hbm, query_gain, key_gain, bucket_hbm,
                 frames_hbm, result,
                 feat, taps_ref, bias, embed, gains, bucket, frames, key_rows, halo_out, halo_in,
                 xbuf, pick_out, pick_in, ysum, ybuf, part_now, queries, keys, values, ones, soft,
                 load_sem, halo_ssem, halo_rsem, x_ssem, x_rsem, c_ssem, c_rsem, y_ssem, y_rsem, relay):
    tile = lax.axis_index("tile")
    seq = lax.axis_index("seq")
    group = lax.axis_index("group")
    n_tile = lax.axis_size("tile")
    x_at = group // 4
    hi_at = (group // 2) % 2
    core_at = group % 2

    def at_x(step):
        return {"group": ((x_at + step) % N_X) * 4 + hi_at * 2 + core_at}

    def at_y(step_hi, step_tile):
        return {"tile": (tile + step_tile) % n_tile,
                "group": x_at * 4 + ((hi_at + step_hi) % 2) * 2 + core_at}

    partner = {"group": x_at * 4 + hi_at * 2 + (1 - core_at)}
    x_steps = (4, 3, 5, 2, 6, 1, 7)
    y_steps = [(1, 0), (1, 1), (1, 3), (1, 2), (0, 2), (0, 1), (0, 3)]

    loads = [
        pltpu.make_async_copy(source, target, load_sem.at[at])
        for at, (source, target) in enumerate((
            (taps_hbm, taps_ref), (feat_hbm, feat), (bias_hbm, bias), (bucket_hbm, bucket),
            (frames_hbm, frames), (embed_hbm, embed), (query_gain, gains.at[0]),
            (key_gain, gains.at[1])))
    ]
    for load in loads:
        load.start()
    next_x = [at_x(1), at_x(N_X - 1)]
    next_y = [
        {"tile": (tile + 1) % n_tile,
         "group": x_at * 4 + ((hi_at + (tile + 1) // 4) % 2) * 2 + core_at},
        {"tile": (tile + n_tile - 1) % n_tile,
         "group": x_at * 4 + ((hi_at + (4 - tile) // 4) % 2) * 2 + core_at},
    ]
    barrier = pltpu.get_barrier_semaphore()
    for near in next_x + next_y + [partner]:
        pl.semaphore_signal(barrier, inc=1, device_id=near, device_id_type=MESH)

    def tell(ring, k):
        for near in (next_x, next_y)[ring]:
            pl.semaphore_signal(
                relay.at[ring, k], inc=1, device_id=near, device_id_type=MESH)

    def hear_all(ring):
        for k in range(3):
            pl.semaphore_wait(relay.at[ring, k], 2)
            if k < 2:
                tell(ring, k + 1)

    xbuf[N_X] = jnp.zeros((64, 128), jnp.bfloat16)
    for load in loads[:2]:
        load.wait()
    taps = taps_ref[...]
    first_frame = feat[0].reshape(256, 512)
    second_frame = feat[1].reshape(256, 512)
    from_first = dot(taps, first_frame, ((1,), (1,)))
    from_second = dot(taps[288:], second_frame, ((1,), (1,)))
    both = from_first[:144] + from_first[144:288]
    frame_sums = (both + from_first[288:], both + from_second)

    lane = lax.broadcasted_iota(jnp.int32, (ZC, 128), 1)
    column = lane % 64
    low_half = lane < 64

    def columns(sums, row_tap, pair):
        def at(col_tap):
            begin = (row_tap * 3 + col_tap) * ZC
            return sums[begin : begin + ZC, pair * 128 : pair * 128 + 128]

        left, middle, right = at(0), at(1), at(2)
        left = jnp.where(column == 0, left, pltpu.roll(left, 1, 1))
        right = jnp.where(column == 63, right, pltpu.roll(right, 127, 1))
        return left + middle + right

    part = [[[columns(frame_sums[f], row_tap, pair) for pair in range(2)]
             for row_tap in range(3)] for f in range(2)]

    def swap(value):
        return pltpu.roll(value, 64, 1)

    up, down = 0, 2
    halo_out[0] = jnp.where(low_half, part[0][down][0], swap(part[1][down][0]))
    halo_out[1] = jnp.where(low_half, swap(part[0][up][1]), part[1][up][1])
    halo_in[0] = jnp.where(low_half, part[0][up][0], swap(part[1][up][0]))
    halo_in[1] = jnp.where(low_half, swap(part[0][down][1]), part[1][down][1])

    pl.semaphore_wait(barrier, 5)

    to_prev = pltpu.make_async_remote_copy(
        src_ref=halo_out.at[0], dst_ref=halo_in.at[3], send_sem=halo_ssem.at[0],
        recv_sem=halo_rsem.at[0], device_id={"tile": (tile + n_tile - 1) % n_tile},
        device_id_type=MESH)
    to_next = pltpu.make_async_remote_copy(
        src_ref=halo_out.at[1], dst_ref=halo_in.at[2], send_sem=halo_ssem.at[1],
        recv_sem=halo_rsem.at[1], device_id={"tile": (tile + 1) % n_tile},
        device_id_type=MESH)
    has_prev = tile > 0
    has_next = tile < n_tile - 1

    @pl.when(has_prev)
    def _():
        to_prev.start()

    @pl.when(has_next)
    def _():
        to_next.start()

    tell(0, 0)
    tell(1, 0)

    for load in loads[2:5]:
        load.wait()
    buckets = [x_at * 4 + ((hi_at + d_hi) % 2) * 2 + (core_at + d_core) % 2
               for d_hi in range(2) for d_core in range(2)]

    def scan_slot(g, carry):
        here = bucket[seq, g]
        done = []
        for at, wanted in enumerate(buckets):
            first, second, count = carry[3 * at : 3 * at + 3]
            hit = here == wanted
            first = jnp.where(hit & (count == 0), g, first)
            second = jnp.where(hit & (count == 1), g, second)
            count = count + jnp.where(hit, 1, 0)
            done += [first, second, count]
        return tuple(done)

    slots = lax.fori_loop(0, 32, scan_slot, (jnp.int32(0),) * 12)

    bias_column = jnp.zeros((ZC, 128), jnp.float32)
    channel = lax.broadcasted_iota(jnp.int32, (ZC, 128), 0)
    for k in range(ZC):
        bias_column = jnp.where(channel == k, bias[k], bias_column)

    hear_all(0)

    @pl.when(has_prev)
    def _():
        to_next.wait_recv()

    @pl.when(has_next)
    def _():
        to_prev.wait_recv()

    top = halo_in[jnp.where(has_prev, 2, 0)]
    bottom = halo_in[jnp.where(has_next, 3, 1)]
    latent = []
    for f in range(2):
        top_f = top if f == 0 else swap(top)
        bottom_f = swap(bottom) if f == 0 else bottom
        above = [swap(part[f][up][pair]) for pair in range(2)]
        below = [swap(part[f][down][pair]) for pair in range(2)]
        shifted_up = (jnp.where(low_half, top_f, above[0]), jnp.where(low_half, above[0], above[1]))
        shifted_down = (jnp.where(low_half, below[0], below[1]), jnp.where(low_half, below[1], bottom_f))
        for pair in range(2):
            total = shifted_up[pair] + part[f][1][pair] + shifted_down[pair] + bias_column
            latent.append(total.astype(jnp.bfloat16))

    rows_at = lax.broadcasted_iota(jnp.int32, (128, 128), 0)
    lanes_at = lax.broadcasted_iota(jnp.int32, (128, 128), 1)
    wanted_row = (lanes_at // 64) * 64 + (lanes_at % 32) * 2 + (lanes_at // 32) % 2
    selector = jnp.where(rows_at == wanted_row, 1.0, 0.0).astype(jnp.bfloat16)
    chosen = dot(jnp.concatenate(latent, axis=0), selector)
    block = lane // 32
    patch_rows = []
    for yx in range(4):
        merged = jnp.zeros((ZC, 128), jnp.float32)
        for fi in range(4):
            piece = chosen[fi * ZC : fi * ZC + ZC]
            if fi != yx:
                piece = pltpu.roll(piece, ((fi - yx) % 4) * 32, 1)
            merged = jnp.where(block == fi, piece, merged)
        patch_rows.append(merged)
    xbuf[0] = jnp.concatenate(patch_rows, axis=0).astype(jnp.bfloat16)

    x_copies = []
    for step in (4, 3, 5, 2, 6, 1, 7):
        copy = pltpu.make_async_remote_copy(
            src_ref=xbuf.at[0], dst_ref=xbuf.at[step], send_sem=x_ssem.at[step],
            recv_sem=x_rsem.at[step], device_id=at_x(step), device_id_type=MESH)
        copy.start()
        x_copies.append(copy)

    picks = []
    for at in range(4):
        first, second, count = slots[3 * at : 3 * at + 3]
        for slot, source in enumerate((first, second)):
            mine = (count > slot) & (source % 4 == hi_at * 2 + core_at)
            picks.append(jnp.where(mine, (x_at + N_X - source // 4) % N_X, N_X))

    hear_all(1)
    for load in loads[5:]:
        load.wait()
    for at in range(HEADS):
        piece = embed[:, D + at * HEAD : D + at * HEAD + HEAD]
        key_rows[at * HEAD : at * HEAD + HEAD] = piece.astype(jnp.float32).T.astype(jnp.bfloat16)
    gain = gains[0] * gains[1] * (math.log2(math.e) / math.sqrt(HEAD))
    token = lax.broadcasted_iota(jnp.int32, (128, HEAD), 0)
    valid = []
    for slot in range(CAP):
        first, second, count = slots[:3]
        total = jnp.where(count > slot, frames[seq, second if slot else first], 0)
        keep = token // 64 < total
        valid.append(keep)
        ones[slot] = jnp.where(keep, 1.0, 0.0).astype(jnp.bfloat16)

    for copy in x_copies:
        copy.wait_recv()

    for d_hi in range(2):
        for slot in range(CAP):
            pick_out[d_hi, slot] = xbuf[picks[(d_hi * 2 + 1) * 2 + slot]]
    across = pltpu.make_async_remote_copy(
        src_ref=pick_out, dst_ref=pick_in, send_sem=c_ssem.at[0], recv_sem=c_rsem.at[0],
        device_id=partner, device_id_type=MESH)
    across.start()
    own = [[xbuf[picks[d_hi * 4 + slot]] for slot in range(CAP)] for d_hi in range(2)]
    across.wait_recv()
    for d_hi in range(2):
        for slot in range(CAP):
            ysum[d_hi, slot] = own[d_hi][slot] + pick_in[d_hi, slot]

    y_copies = []
    for d_hi, d_tile in y_steps:
        at = d_hi * 4 + d_tile
        copy = pltpu.make_async_remote_copy(
            src_ref=ysum.at[d_hi], dst_ref=ybuf.at[at], send_sem=y_ssem.at[at],
            recv_sem=y_rsem.at[at], device_id=at_y(d_hi, d_tile), device_id_type=MESH)
        copy.start()
        y_copies.append(copy)
    arrivals = {step: copy for step, copy in zip(y_steps, y_copies)}
    turns = ((2, 3, 0, 1), (2, 3, 1, 0), (2, 3, 0, 1), (2, 3, 0, 1))

    def take(d_tile):
        arrivals[1, d_tile].wait_recv()
        if d_tile:
            arrivals[0, d_tile].wait_recv()
        near = ybuf if d_tile else ysum
        for slot in range(CAP):
            part_now[slot] = near[d_tile, slot] + ybuf[4 + d_tile, slot]

    def make_queries():
        for slot in range(CAP):
            u = dot(part_now[slot].astype(jnp.float32).T.astype(jnp.bfloat16), embed[:, :D])
            for at in range(HEADS):
                mine = u[:, at * HEAD : at * HEAD + HEAD]
                mean = jnp.mean(mine * mine, axis=1, keepdims=True)
                queries[slot, at] = (mine * lax.rsqrt(mean + 1e-6) * gain).astype(jnp.bfloat16)

    for turn in range(4):
        for here in range(4):
            pl.when(tile == here)(functools.partial(take, (here - turns[here][turn]) % 4))
        own_turn = {0: tile == 2, 1: tile == 3, 2: tile < 2}
        if turn in own_turn:
            pl.when(own_turn[turn])(make_queries)
        parts = [part_now[slot] for slot in range(CAP)]
        joined = jnp.concatenate(parts, axis=1)
        for at in range(HEADS):
            u = dot(key_rows[at * HEAD : at * HEAD + HEAD], joined)
            mean = jnp.mean(u * u, axis=0, keepdims=True)
            keys[turn, at] = (u * lax.rsqrt(mean + 1e-6)).astype(jnp.bfloat16)
        tall = jnp.concatenate(
            [jnp.where(valid[slot][:, :64], parts[slot].astype(jnp.float32).T, 0.0)
             for slot in range(CAP)], axis=0
        ).astype(jnp.bfloat16)
        for at in range(0, HEADS, 2):
            begin = 2 * D + at * HEAD
            v = dot(tall, embed[:, begin : begin + 2 * HEAD]).astype(jnp.bfloat16)
            values[turn, at] = v[:, :HEAD]
            values[turn, at + 1] = v[:, HEAD:]

    units = [(at, slot) for at in range(HEADS) for slot in range(CAP)]
    for turn in range(len(units) + 1):
        if turn < len(units):
            at, slot = units[turn]
            begin = slot * HEAD
            k = jnp.concatenate(
                [keys[part, at, :, begin : begin + HEAD] for part in range(4)], axis=1)
            soft[turn % 3] = jnp.exp2(dot(queries[slot, at], k)).astype(jnp.bfloat16)
        if turn:
            at, slot = units[turn - 1]
            begin = slot * HEAD
            v = jnp.concatenate(
                [jnp.concatenate([values[part, at, begin : begin + HEAD], ones[slot]], axis=1)
                 for part in range(4)], axis=0)
            mixed = dot(soft[(turn - 1) % 3], v)
            final = jnp.where(valid[slot], mixed[:, :HEAD] / mixed[:, HEAD:], 0.0)
            result[0, 0, slot, :, at * HEAD : at * HEAD + HEAD] = final.astype(jnp.bfloat16)

    @pl.when(has_prev)
    def _():
        to_prev.wait_send()

    @pl.when(has_next)
    def _():
        to_next.wait_send()

    for copy in x_copies:
        copy.wait_send()
    across.wait_send()
    for copy in y_copies:
        copy.wait_send()


def fused(features, taps, bias, embed, query_gain, key_gain, bucket, frames):
    anywhere = pl.BlockSpec(memory_space=pltpu.HBM)
    vector = pl.BlockSpec(memory_space=pltpu.VMEM)
    return pl.pallas_call(
        fused_kernel,
        out_shape=pltpu.VMEM((1, 1, CAP, 128, D), jnp.bfloat16),
        in_specs=[anywhere] * 8,
        out_specs=vector,
        scratch_shapes=[
            pltpu.VMEM((2, 4, 64, 512), jnp.bfloat16),
            pltpu.VMEM((432, 512), jnp.bfloat16),
            pltpu.SMEM((ZC,), jnp.float32),
            pltpu.VMEM((64, 3 * D), jnp.bfloat16),
            pltpu.VMEM((2, 1, HEAD), jnp.float32),
            pltpu.SMEM((8, 32), jnp.int32),
            pltpu.SMEM((8, 32), jnp.int32),
            pltpu.VMEM((D, 64), jnp.bfloat16),
            pltpu.VMEM((2, ZC, 128), jnp.float32),
            pltpu.VMEM((4, ZC, 128), jnp.float32),
            pltpu.VMEM((N_X + 1, 64, 128), jnp.bfloat16),
            pltpu.VMEM((2, CAP, 64, 128), jnp.bfloat16),
            pltpu.VMEM((2, CAP, 64, 128), jnp.bfloat16),
            pltpu.VMEM((2, CAP, 64, 128), jnp.bfloat16),
            pltpu.VMEM((8, CAP, 64, 128), jnp.bfloat16),
            pltpu.VMEM((CAP, 64, 128), jnp.bfloat16),
            pltpu.VMEM((CAP, HEADS, 128, HEAD), jnp.bfloat16),
            pltpu.VMEM((4, HEADS, HEAD, CAP * 128), jnp.bfloat16),
            pltpu.VMEM((4, HEADS, CAP * 128, HEAD), jnp.bfloat16),
            pltpu.VMEM((CAP, 128, HEAD), jnp.bfloat16),
            pltpu.VMEM((3, 128, 512), jnp.bfloat16),
            pltpu.SemaphoreType.DMA((8,)),
            pltpu.SemaphoreType.DMA((2,)),
            pltpu.SemaphoreType.DMA((2,)),
            pltpu.SemaphoreType.DMA((N_X,)),
            pltpu.SemaphoreType.DMA((N_X,)),
            pltpu.SemaphoreType.DMA((1,)),
            pltpu.SemaphoreType.DMA((1,)),
            pltpu.SemaphoreType.DMA((8,)),
            pltpu.SemaphoreType.DMA((8,)),
            pltpu.SemaphoreType.REGULAR((2, 3)),
        ],
        compiler_params=pltpu.CompilerParams(
            collective_id=0, has_side_effects=True, vmem_limit_bytes=40 * 2**20),
        name="fused",
    )(*(pltpu.with_memory_space_constraint(array, pltpu.HBM) for array in (
        features, taps, bias, embed, query_gain, key_gain, bucket, frames)))


def shards(features, conv_weight, conv_bias, embed_qkv, query_gain, key_gain, bucket, frames):
    taps = jnp.transpose(conv_weight, (0, 1, 2, 4, 3)).reshape(432, 512)
    return fused(
        features[0, 0], taps, conv_bias, embed_qkv, query_gain.reshape(1, HEAD),
        key_gain.reshape(1, HEAD), bucket, frames
    )


def solution(mesh):
    in_specs = (P("seq", "group", None, "tile", None, None), P(), P(), P(), P(), P(), P(), P())
    out_specs = P("seq", "group", None, "tile", None)
    return jax.shard_map(shards, mesh=mesh, in_specs=in_specs, out_specs=out_specs, check_vma=False)
```

```python
import functools
import math

import jax
import jax.numpy as jnp
from jax import lax
from jax.experimental import pallas as pl
from jax.experimental.pallas import tpu as pltpu
from jax.sharding import PartitionSpec as P

HEADS = 12
HEAD = 128
D = 1536
CAP = 2
N_X = 8
ZC = 16
MESH = pl.DeviceIdType.MESH


def dot(a, b, dims=((1,), (0,))):
    return lax.dot_general(a, b, (dims, ((), ())), preferred_element_type=jnp.float32)


def fused_kernel(feat_hbm, taps_hbm, bias_hbm, embed_hbm, query_gain, key_gain, bucket_hbm,
                 frames_hbm, result,
                 feat, taps_ref, bias, embed, gains, bucket, frames, key_rows, halo_out, halo_in,
                 xbuf, pick_out, pick_in, ysum, ybuf, part_now, queries, keys, values, ones, soft,
                 load_sem, halo_ssem, halo_rsem, x_ssem, x_rsem, c_ssem, c_rsem, y_ssem, y_rsem, relay):
    tile = lax.axis_index("tile")
    seq = lax.axis_index("seq")
    group = lax.axis_index("group")
    n_tile = lax.axis_size("tile")
    x_at = group // 4
    hi_at = (group // 2) % 2
    core_at = group % 2

    def at_x(step):
        return {"group": ((x_at + step) % N_X) * 4 + hi_at * 2 + core_at}

    def at_y(step_hi, step_tile):
        return {"tile": (tile + step_tile) % n_tile,
                "group": x_at * 4 + ((hi_at + step_hi) % 2) * 2 + core_at}

    partner = {"group": x_at * 4 + hi_at * 2 + (1 - core_at)}
    x_steps = (4, 3, 5, 2, 6, 1, 7)
    y_steps = [(1, 0), (1, 1), (1, 3), (1, 2), (0, 2), (0, 1), (0, 3)]

    loads = [
        pltpu.make_async_copy(source, target, load_sem.at[at])
        for at, (source, target) in enumerate((
            (taps_hbm, taps_ref), (feat_hbm, feat), (bias_hbm, bias), (bucket_hbm, bucket),
            (frames_hbm, frames), (embed_hbm, embed), (query_gain, gains.at[0]),
            (key_gain, gains.at[1])))
    ]
    for load in loads:
        load.start()
    next_y = [
        {"tile": (tile + 1) % n_tile,
         "group": x_at * 4 + ((hi_at + (tile + 1) // 4) % 2) * 2 + core_at},
        {"tile": (tile + n_tile - 1) % n_tile,
         "group": x_at * 4 + ((hi_at + (4 - tile) // 4) % 2) * 2 + core_at},
    ]
    barrier = pltpu.get_barrier_semaphore()
    for near in [at_x(step) for step in x_steps] + next_y + [partner]:
        pl.semaphore_signal(barrier, inc=1, device_id=near, device_id_type=MESH)

    def tell(k):
        for near in next_y:
            pl.semaphore_signal(relay.at[k], inc=1, device_id=near, device_id_type=MESH)

    xbuf[N_X] = jnp.zeros((64, 128), jnp.bfloat16)
    for load in loads[:2]:
        load.wait()
    taps = taps_ref[...]
    first_frame = feat[0].reshape(256, 512)
    second_frame = feat[1].reshape(256, 512)
    from_first = dot(taps, first_frame, ((1,), (1,)))
    from_second = dot(taps[288:], second_frame, ((1,), (1,)))
    both = from_first[:144] + from_first[144:288]
    frame_sums = (both + from_first[288:], both + from_second)

    lane = lax.broadcasted_iota(jnp.int32, (ZC, 128), 1)
    column = lane % 64
    low_half = lane < 64

    def columns(sums, row_tap, pair):
        def at(col_tap):
            begin = (row_tap * 3 + col_tap) * ZC
            return sums[begin : begin + ZC, pair * 128 : pair * 128 + 128]

        left, middle, right = at(0), at(1), at(2)
        left = jnp.where(column == 0, left, pltpu.roll(left, 1, 1))
        right = jnp.where(column == 63, right, pltpu.roll(right, 127, 1))
        return left + middle + right

    part = [[[columns(frame_sums[f], row_tap, pair) for pair in range(2)]
             for row_tap in range(3)] for f in range(2)]

    def swap(value):
        return pltpu.roll(value, 64, 1)

    up, down = 0, 2
    halo_out[0] = jnp.where(low_half, part[0][down][0], swap(part[1][down][0]))
    halo_out[1] = jnp.where(low_half, swap(part[0][up][1]), part[1][up][1])
    halo_in[0] = jnp.where(low_half, part[0][up][0], swap(part[1][up][0]))
    halo_in[1] = jnp.where(low_half, swap(part[0][down][1]), part[1][down][1])

    pl.semaphore_wait(barrier, 10)

    to_prev = pltpu.make_async_remote_copy(
        src_ref=halo_out.at[0], dst_ref=halo_in.at[3], send_sem=halo_ssem.at[0],
        recv_sem=halo_rsem.at[0], device_id={"tile": (tile + n_tile - 1) % n_tile},
        device_id_type=MESH)
    to_next = pltpu.make_async_remote_copy(
        src_ref=halo_out.at[1], dst_ref=halo_in.at[2], send_sem=halo_ssem.at[1],
        recv_sem=halo_rsem.at[1], device_id={"tile": (tile + 1) % n_tile},
        device_id_type=MESH)
    has_prev = tile > 0
    has_next = tile < n_tile - 1

    @pl.when(has_prev)
    def _():
        to_prev.start()

    @pl.when(has_next)
    def _():
        to_next.start()

    tell(0)

    for load in loads[2:5]:
        load.wait()
    buckets = [x_at * 4 + ((hi_at + d_hi) % 2) * 2 + (core_at + d_core) % 2
               for d_hi in range(2) for d_core in range(2)]

    def scan_slot(g, carry):
        here = bucket[seq, g]
        done = []
        for at, wanted in enumerate(buckets):
            first, second, count = carry[3 * at : 3 * at + 3]
            hit = here == wanted
            first = jnp.where(hit & (count == 0), g, first)
            second = jnp.where(hit & (count == 1), g, second)
            count = count + jnp.where(hit, 1, 0)
            done += [first, second, count]
        return tuple(done)

    slots = lax.fori_loop(0, 32, scan_slot, (jnp.int32(0),) * 12)

    bias_column = jnp.zeros((ZC, 128), jnp.float32)
    channel = lax.broadcasted_iota(jnp.int32, (ZC, 128), 0)
    for k in range(ZC):
        bias_column = jnp.where(channel == k, bias[k], bias_column)

    @pl.when(has_prev)
    def _():
        to_next.wait_recv()

    @pl.when(has_next)
    def _():
        to_prev.wait_recv()

    top = halo_in[jnp.where(has_prev, 2, 0)]
    bottom = halo_in[jnp.where(has_next, 3, 1)]
    latent = []
    for f in range(2):
        top_f = top if f == 0 else swap(top)
        bottom_f = swap(bottom) if f == 0 else bottom
        above = [swap(part[f][up][pair]) for pair in range(2)]
        below = [swap(part[f][down][pair]) for pair in range(2)]
        shifted_up = (jnp.where(low_half, top_f, above[0]), jnp.where(low_half, above[0], above[1]))
        shifted_down = (jnp.where(low_half, below[0], below[1]), jnp.where(low_half, below[1], bottom_f))
        for pair in range(2):
            total = shifted_up[pair] + part[f][1][pair] + shifted_down[pair] + bias_column
            latent.append(total.astype(jnp.bfloat16))

    rows_at = lax.broadcasted_iota(jnp.int32, (128, 128), 0)
    lanes_at = lax.broadcasted_iota(jnp.int32, (128, 128), 1)
    wanted_row = (lanes_at // 64) * 64 + (lanes_at % 32) * 2 + (lanes_at // 32) % 2
    selector = jnp.where(rows_at == wanted_row, 1.0, 0.0).astype(jnp.bfloat16)
    chosen = dot(jnp.concatenate(latent, axis=0), selector)
    block = lane // 32
    patch_rows = []
    for yx in range(4):
        merged = jnp.zeros((ZC, 128), jnp.float32)
        for fi in range(4):
            piece = chosen[fi * ZC : fi * ZC + ZC]
            if fi != yx:
                piece = pltpu.roll(piece, ((fi - yx) % 4) * 32, 1)
            merged = jnp.where(block == fi, piece, merged)
        patch_rows.append(merged)
    xbuf[0] = jnp.concatenate(patch_rows, axis=0).astype(jnp.bfloat16)

    x_copies = []
    for step in (4, 3, 5, 2, 6, 1, 7):
        copy = pltpu.make_async_remote_copy(
            src_ref=xbuf.at[0], dst_ref=xbuf.at[step], send_sem=x_ssem.at[step],
            recv_sem=x_rsem.at[step], device_id=at_x(step), device_id_type=MESH)
        copy.start()
        x_copies.append(copy)

    picks = []
    for at in range(4):
        first, second, count = slots[3 * at : 3 * at + 3]
        for slot, source in enumerate((first, second)):
            mine = (count > slot) & (source % 4 == hi_at * 2 + core_at)
            picks.append(jnp.where(mine, (x_at + N_X - source // 4) % N_X, N_X))

    for k in range(3):
        pl.semaphore_wait(relay.at[k], 2)
        if k < 2:
            tell(k + 1)
    for load in loads[5:]:
        load.wait()
    for at in range(HEADS):
        piece = embed[:, D + at * HEAD : D + at * HEAD + HEAD]
        key_rows[at * HEAD : at * HEAD + HEAD] = piece.astype(jnp.float32).T.astype(jnp.bfloat16)
    gain = gains[0] * gains[1] * (math.log2(math.e) / math.sqrt(HEAD))
    token = lax.broadcasted_iota(jnp.int32, (128, HEAD), 0)
    valid = []
    for slot in range(CAP):
        first, second, count = slots[:3]
        total = jnp.where(count > slot, frames[seq, second if slot else first], 0)
        keep = token // 64 < total
        valid.append(keep)
        ones[slot] = jnp.where(keep, 1.0, 0.0).astype(jnp.bfloat16)

    for copy in x_copies:
        copy.wait_recv()

    for d_hi in range(2):
        for slot in range(CAP):
            pick_out[d_hi, slot] = xbuf[picks[(d_hi * 2 + 1) * 2 + slot]]
    across = pltpu.make_async_remote_copy(
        src_ref=pick_out, dst_ref=pick_in, send_sem=c_ssem.at[0], recv_sem=c_rsem.at[0],
        device_id=partner, device_id_type=MESH)
    across.start()
    own = [[xbuf[picks[d_hi * 4 + slot]] for slot in range(CAP)] for d_hi in range(2)]
    across.wait_recv()
    for d_hi in range(2):
        for slot in range(CAP):
            ysum[d_hi, slot] = own[d_hi][slot] + pick_in[d_hi, slot]

    y_copies = []
    for d_hi, d_tile in y_steps:
        at = d_hi * 4 + d_tile
        copy = pltpu.make_async_remote_copy(
            src_ref=ysum.at[d_hi], dst_ref=ybuf.at[at], send_sem=y_ssem.at[at],
            recv_sem=y_rsem.at[at], device_id=at_y(d_hi, d_tile), device_id_type=MESH)
        copy.start()
        y_copies.append(copy)
    arrivals = {step: copy for step, copy in zip(y_steps, y_copies)}
    turns = ((2, 3, 0, 1), (2, 3, 1, 0), (2, 3, 0, 1), (2, 3, 0, 1))

    def take(d_tile):
        arrivals[1, d_tile].wait_recv()
        if d_tile:
            arrivals[0, d_tile].wait_recv()
        near = ybuf if d_tile else ysum
        for slot in range(CAP):
            part_now[slot] = near[d_tile, slot] + ybuf[4 + d_tile, slot]

    def make_queries():
        for slot in range(CAP):
            u = dot(part_now[slot].astype(jnp.float32).T.astype(jnp.bfloat16), embed[:, :D])
            for at in range(HEADS):
                mine = u[:, at * HEAD : at * HEAD + HEAD]
                mean = jnp.mean(mine * mine, axis=1, keepdims=True)
                queries[slot, at] = (mine * lax.rsqrt(mean + 1e-6) * gain).astype(jnp.bfloat16)

    for turn in range(4):
        for here in range(4):
            pl.when(tile == here)(functools.partial(take, (here - turns[here][turn]) % 4))
        own_turn = {0: tile == 2, 1: tile == 3, 2: tile < 2}
        if turn in own_turn:
            pl.when(own_turn[turn])(make_queries)
        parts = [part_now[slot] for slot in range(CAP)]
        joined = jnp.concatenate(parts, axis=1)
        for at in range(HEADS):
            u = dot(key_rows[at * HEAD : at * HEAD + HEAD], joined)
            mean = jnp.mean(u * u, axis=0, keepdims=True)
            keys[turn, at] = (u * lax.rsqrt(mean + 1e-6)).astype(jnp.bfloat16)
        tall = jnp.concatenate(
            [jnp.where(valid[slot][:, :64], parts[slot].astype(jnp.float32).T, 0.0)
             for slot in range(CAP)], axis=0
        ).astype(jnp.bfloat16)
        for at in range(0, HEADS, 2):
            begin = 2 * D + at * HEAD
            v = dot(tall, embed[:, begin : begin + 2 * HEAD]).astype(jnp.bfloat16)
            values[turn, at] = v[:, :HEAD]
            values[turn, at + 1] = v[:, HEAD:]

    units = [(at, slot) for at in range(HEADS) for slot in range(CAP)]
    for turn in range(len(units) + 1):
        if turn < len(units):
            at, slot = units[turn]
            begin = slot * HEAD
            k = jnp.concatenate(
                [keys[part, at, :, begin : begin + HEAD] for part in range(4)], axis=1)
            soft[turn % 3] = jnp.exp2(dot(queries[slot, at], k)).astype(jnp.bfloat16)
        if turn:
            at, slot = units[turn - 1]
            begin = slot * HEAD
            v = jnp.concatenate(
                [jnp.concatenate([values[part, at, begin : begin + HEAD], ones[slot]], axis=1)
                 for part in range(4)], axis=0)
            mixed = dot(soft[(turn - 1) % 3], v)
            final = jnp.where(valid[slot], mixed[:, :HEAD] / mixed[:, HEAD:], 0.0)
            result[0, 0, slot, :, at * HEAD : at * HEAD + HEAD] = final.astype(jnp.bfloat16)

    @pl.when(has_prev)
    def _():
        to_prev.wait_send()

    @pl.when(has_next)
    def _():
        to_next.wait_send()

    for copy in x_copies:
        copy.wait_send()
    across.wait_send()
    for copy in y_copies:
        copy.wait_send()


def fused(features, taps, bias, embed, query_gain, key_gain, bucket, frames):
    anywhere = pl.BlockSpec(memory_space=pltpu.HBM)
    vector = pl.BlockSpec(memory_space=pltpu.VMEM)
    return pl.pallas_call(
        fused_kernel,
        out_shape=pltpu.VMEM((1, 1, CAP, 128, D), jnp.bfloat16),
        in_specs=[anywhere] * 8,
        out_specs=vector,
        scratch_shapes=[
            pltpu.VMEM((2, 4, 64, 512), jnp.bfloat16),
            pltpu.VMEM((432, 512), jnp.bfloat16),
            pltpu.SMEM((ZC,), jnp.float32),
            pltpu.VMEM((64, 3 * D), jnp.bfloat16),
            pltpu.VMEM((2, 1, HEAD), jnp.float32),
            pltpu.SMEM((8, 32), jnp.int32),
            pltpu.SMEM((8, 32), jnp.int32),
            pltpu.VMEM((D, 64), jnp.bfloat16),
            pltpu.VMEM((2, ZC, 128), jnp.float32),
            pltpu.VMEM((4, ZC, 128), jnp.float32),
            pltpu.VMEM((N_X + 1, 64, 128), jnp.bfloat16),
            pltpu.VMEM((2, CAP, 64, 128), jnp.bfloat16),
            pltpu.VMEM((2, CAP, 64, 128), jnp.bfloat16),
            pltpu.VMEM((2, CAP, 64, 128), jnp.bfloat16),
            pltpu.VMEM((8, CAP, 64, 128), jnp.bfloat16),
            pltpu.VMEM((CAP, 64, 128), jnp.bfloat16),
            pltpu.VMEM((CAP, HEADS, 128, HEAD), jnp.bfloat16),
            pltpu.VMEM((4, HEADS, HEAD, CAP * 128), jnp.bfloat16),
            pltpu.VMEM((4, HEADS, CAP * 128, HEAD), jnp.bfloat16),
            pltpu.VMEM((CAP, 128, HEAD), jnp.bfloat16),
            pltpu.VMEM((3, 128, 512), jnp.bfloat16),
            pltpu.SemaphoreType.DMA((8,)),
            pltpu.SemaphoreType.DMA((2,)),
            pltpu.SemaphoreType.DMA((2,)),
            pltpu.SemaphoreType.DMA((N_X,)),
            pltpu.SemaphoreType.DMA((N_X,)),
            pltpu.SemaphoreType.DMA((1,)),
            pltpu.SemaphoreType.DMA((1,)),
            pltpu.SemaphoreType.DMA((8,)),
            pltpu.SemaphoreType.DMA((8,)),
            pltpu.SemaphoreType.REGULAR((3,)),
        ],
        compiler_params=pltpu.CompilerParams(
            collective_id=0, has_side_effects=True, vmem_limit_bytes=40 * 2**20),
        name="fused",
    )(*(pltpu.with_memory_space_constraint(array, pltpu.HBM) for array in (
        features, taps, bias, embed, query_gain, key_gain, bucket, frames)))


def shards(features, conv_weight, conv_bias, embed_qkv, query_gain, key_gain, bucket, frames):
    taps = jnp.transpose(conv_weight, (0, 1, 2, 4, 3)).reshape(432, 512)
    return fused(
        features[0, 0], taps, conv_bias, embed_qkv, query_gain.reshape(1, HEAD),
        key_gain.reshape(1, HEAD), bucket, frames
    )


def solution(mesh):
    in_specs = (P("seq", "group", None, "tile", None, None), P(), P(), P(), P(), P(), P(), P())
    out_specs = P("seq", "group", None, "tile", None)
    return jax.shard_map(shards, mesh=mesh, in_specs=in_specs, out_specs=out_specs, check_vma=False)
```
